32 devices in a mesh: pts: 8 (over y, x, core), freq: 4 (over z).
Axes of the slice: x: 2, y: 2, z: 4, core: 2. Of those that a mesh axis runs over, the one named last changes fastest.
Arguments:
- spectra: bfloat16 [128, 2, 32, 16384], P('freq', None, None, 'pts'), may hold values from -6 to 6
- weights: float32 [16384], P('pts'), may hold values from 0.25 to 4
- triads: int32 [64, 2], replicated, may hold values from 0 to 127, as said below
Outputs:
- bispectrum: float32 [64, 2, 32, 32], P('freq')
- density: float32 [128, 2, 32, 32], P('freq')
- vectors: float32 [64, 2, 32], P('freq')
- energy: float32 [64], P('freq')
- mode_fields: float32 [64, 2, 16384], P('freq', None, 'pts')
The draws below stay inside these ranges and needn't reach their ends.
Inputs may be any that keep to these rules, and one draw needn't show every extreme that they name: Row t holds (k, l) of triad t. The triads of group g, rows g * 16 to (g + 1) * 16 - 1, have k within the group's own frequencies g * 32 to (g + 1) * 32 - 1. The l of exactly 4 triads of each group lie in each group's frequency range. Among the 32 frequencies l and (k + l) mod 128 of one group's triads, at most 12 lie in any one group's range, and in every group some range holds exactly 12.
All inputs are finite; a program needn't handle non-finite values.
Results may differ from the reference program's by a relative error of at most 0.0052.
Values may be sent and summed in bfloat16 or wider, within the bound.
A program may use at most 128 MiB of HBM per device.

```python
import math
import jax
import jax.numpy as jnp
from jax import lax

F = 128
NB = 32
TRI_G = 16
ITERS = 3
NPTS = 16384
N_FREQ = 4


def draw_triads(key, part):
    f_dev = F // N_FREQ
    key_list = jax.random.split(jax.random.fold_in(key, 11), 7)
    group_ids = jnp.arange(N_FREQ, dtype=jnp.int32)[:, None]
    base_owner = jnp.arange(TRI_G, dtype=jnp.int32) % N_FREQ

    def shuffle_owner(subkey):
        return jax.random.permutation(subkey, base_owner)
    owner_l = jax.vmap(shuffle_owner)(jax.random.split(key_list[0], N_FREQ)).astype(jnp.int32)
    target = jax.random.randint(key_list[1], (N_FREQ, 1), 0, N_FREQ, dtype=jnp.int32)
    coin_flip = jax.random.randint(key_list[2], (N_FREQ, TRI_G), 0, 2, dtype=jnp.int32)
    before_target = (target + N_FREQ - 1) % N_FREQ
    carry_bit = jnp.where(owner_l == target, 0, jnp.where(owner_l == before_target, 1, coin_flip))
    low_k = jax.random.randint(key_list[3], (N_FREQ, TRI_G), 0, f_dev, dtype=jnp.int32)
    high_k = jax.random.randint(key_list[4], (N_FREQ, TRI_G), 1, f_dev, dtype=jnp.int32)
    rest_k = jnp.where(carry_bit == 1, high_k, low_k)
    lower_end = jnp.where(carry_bit == 1, f_dev - rest_k, 0)
    upper_end = jnp.where(carry_bit == 1, f_dev, f_dev - rest_k)
    rest_l = jax.random.randint(key_list[5], (N_FREQ, TRI_G), lower_end, upper_end, dtype=jnp.int32)
    freq_first = group_ids * f_dev + rest_k
    freq_second = owner_l * f_dev + rest_l
    return jnp.stack([freq_first, freq_second], axis=-1).reshape(N_FREQ * TRI_G, 2).astype(jnp.int32)


def shard_levels(stream_key, dims, cuts, least, high):
    def one(position, shards_of):
        steps = jax.random.uniform(jax.random.fold_in(jax.random.fold_in(stream_key, 6), position), (shards_of,), jnp.float32, least / len(cuts), high / len(cuts))
        return jnp.repeat(jnp.exp(steps), dims[position] // shards_of).reshape((-1,) + (1,) * (len(dims) - position - 1))

    factor_of = one(*cuts[0])
    for cut in cuts[1:]:
        factor_of = factor_of * one(*cut)
    return factor_of


def scatter_about(own_key, shape, spread, most, cuts=(), held_as=jnp.bfloat16):
    drawn = spread * jax.random.normal(own_key, shape, jnp.float32)
    if cuts:
        drawn = drawn * shard_levels(own_key, shape, cuts, -0.22, 0.18)
    return jnp.clip(drawn, -most, most).astype(held_as)


def setup_inputs(seed: int = 0) -> dict:
    keys = jax.random.split(jax.random.key(seed), 4)
    spectra = scatter_about(keys[0], (F, 2, NB, NPTS), 1.0, 6.0, ((0, 4), (3, 8)))
    weights = jnp.clip(jnp.exp(math.log(4.0) - 2.7725887 * jax.random.uniform(keys[1], (NPTS,), jnp.float32) ** shard_levels(keys[1], (NPTS,), ((0, 8),), -0.2, 0.2)), 0.25, 4.0)
    triads = draw_triads(jax.random.fold_in(keys[3], 71), 0)
    return {"spectra": spectra, "weights": weights, "triads": triads}


highest = lax.Precision.HIGHEST

def pair_gram(left, right):
    half_rows = left.shape[1]
    flat_left = left.reshape(2 * half_rows, left.shape[2])
    flat_right = right.reshape(2 * half_rows, right.shape[2])
    joined = jnp.dot(flat_left, flat_right.T, preferred_element_type=jnp.float32)
    real_part = joined[:half_rows, :half_rows] + joined[half_rows:, half_rows:]
    imag_part = joined[:half_rows, half_rows:] - joined[half_rows:, :half_rows]
    return jnp.stack([real_part, imag_part])

def weighted_product(first_rows, second_rows, weights):
    first_real = first_rows[0].astype(jnp.float32)
    first_imag = first_rows[1].astype(jnp.float32)
    second_real = second_rows[0].astype(jnp.float32)
    second_imag = second_rows[1].astype(jnp.float32)
    prod_real = first_real * second_real - first_imag * second_imag
    prod_imag = first_real * second_imag + first_imag * second_real
    return (jnp.stack([prod_real, prod_imag]) * weights).astype(jnp.bfloat16)

def apply_matrix(matrix, vector):
    return jnp.einsum('...ab,...b->...a', matrix, vector, precision=highest)

def apply_adjoint(matrix, vector):
    return jnp.einsum('...ba,...b->...a', matrix, vector, precision=highest)

def power_iteration(bispec):
    real_mat = bispec[..., 0, :, :]
    imag_mat = bispec[..., 1, :, :]
    order = real_mat.shape[-1]
    vec_real = jnp.full(real_mat.shape[:-1], 1.0 / math.sqrt(order), jnp.float32)
    vec_imag = jnp.zeros(real_mat.shape[:-1], jnp.float32)
    for sweep_index in range(ITERS):
        out_real = apply_matrix(real_mat, vec_real) - apply_matrix(imag_mat, vec_imag)
        out_imag = apply_matrix(real_mat, vec_imag) + apply_matrix(imag_mat, vec_real)
        back_real = apply_adjoint(real_mat, out_real) + apply_adjoint(imag_mat, out_imag)
        back_imag = apply_adjoint(real_mat, out_imag) - apply_adjoint(imag_mat, out_real)
        factor = 1.0 / jnp.sqrt(lax.optimization_barrier(jnp.sum(back_real * back_real + back_imag * back_imag, axis=-1)) + 1.0)
        vec_real = back_real * factor[..., None]
        vec_imag = back_imag * factor[..., None]
    out_real = apply_matrix(real_mat, vec_real) - apply_matrix(imag_mat, vec_imag)
    out_imag = apply_matrix(real_mat, vec_imag) + apply_matrix(imag_mat, vec_real)
    top_part = lax.optimization_barrier(jnp.sum(out_real * out_real + out_imag * out_imag, axis=-1))
    bottom_part = order * (lax.optimization_barrier(jnp.sum(vec_real * vec_real + vec_imag * vec_imag, axis=-1)) + 1.0)
    return (jnp.stack([vec_real, vec_imag], axis=-2), top_part / bottom_part)

def reference(spectra, weights, triads):
    point_count = spectra.shape[-1]
    blocks = spectra.shape[2]
    k_index = triads[:, 0].astype(jnp.int32)
    l_index = triads[:, 1].astype(jnp.int32)
    m_index = ((k_index + l_index) % F).astype(jnp.int32)

    def one_triad(indices):
        first_rows = lax.dynamic_index_in_dim(spectra, indices[0], 0, keepdims=False)
        second_rows = lax.dynamic_index_in_dim(spectra, indices[1], 0, keepdims=False)
        third_rows = lax.dynamic_index_in_dim(spectra, indices[2], 0, keepdims=False)
        return pair_gram(weighted_product(first_rows, second_rows, weights), third_rows)
    raw_sums = lax.map(one_triad, (k_index, l_index, m_index))
    bispectrum = raw_sums * (1.0 / math.sqrt(blocks * point_count))

    def one_freq(rows):
        weighted = (rows.astype(jnp.float32) * weights).astype(jnp.bfloat16)
        return pair_gram(weighted, rows)
    density = lax.map(one_freq, spectra) * (1.0 / point_count)
    vectors, energy = power_iteration(bispectrum)
    vector_low = vectors.astype(jnp.bfloat16)

    def one_mode(inputs):
        third_rows = lax.dynamic_index_in_dim(spectra, inputs[0], 0, keepdims=False)
        mixed = jnp.einsum('cbp,db->cdp', third_rows.astype(jnp.float32), inputs[1].astype(jnp.float32), precision=highest)
        return jnp.stack([mixed[0, 0] - mixed[1, 1], mixed[0, 1] + mixed[1, 0]])
    mode_fields = lax.map(one_mode, (m_index, vector_low))
    return (bispectrum, density, vectors, energy, mode_fields)
```

```python
import functools
import math

import jax
import jax.numpy as jnp
from jax import lax
from jax.experimental import pallas as pl
from jax.experimental.pallas import tpu as pltpu
from jax.sharding import PartitionSpec as P

ITERS = 3
MESH = pl.DeviceIdType.MESH
f32 = jnp.float32
bf16 = jnp.bfloat16


def gram_pair(left_real, left_imag, right_real, right_imag):
    left = jnp.concatenate([left_real, left_imag], axis=1)
    right = jnp.concatenate(
        [
            jnp.concatenate([right_real, right_imag], axis=1),
            jnp.concatenate([right_imag, -right_real], axis=1),
        ],
        axis=0,
    )
    return lax.dot_general(left, right, (((1,), (1,)), ((), ())), preferred_element_type=f32)


def lane_in(shape):
    return lax.broadcasted_iota(jnp.int32, shape, len(shape) - 1)


def segment_sum(values, low):
    first = jnp.sum(jnp.where(low, values, 0.0), axis=-1, keepdims=True)
    second = jnp.sum(jnp.where(low, 0.0, values), axis=-1, keepdims=True)
    return first, second


def swap_parts(values, is_real):
    axis = values.ndim - 1
    up = pltpu.roll(values, 96, axis)
    down = pltpu.roll(values, 32, axis)
    return jnp.where(is_real, up, down)


def kernel(
    groups,
    point_devs,
    chunks,
    tri_ref,
    w_ref,
    spec_ref,
    bis_out,
    dens_out,
    vec_out,
    energy_out,
    mode_out,
    own,
    acc,
    r1,
    s1,
    r2,
    fin,
    full,
    dacc,
    rd,
    dfin,
    dfull,
    lhs_mine,
    lhs_all,
    modes,
    mode_buf,
    own_sem,
    loc_sem,
    main_send,
    main_recv,
    d1_send,
    d1_recv,
    d2_send,
    d2_recv,
    r1_send,
    r1_recv,
    r2_send,
    r2_recv,
    r3_send,
    r3_recv,
    l_send,
    l_recv,
    m_send,
    m_recv,
    *bufs,
):
    z = lax.axis_index("freq")
    q = lax.axis_index("pts")
    f_dev, _, blocks, points = spec_ref.shape
    width = points // groups
    cw = width // chunks
    triads = tri_ref.shape[0]
    f_total = f_dev * groups
    per_group = triads // groups
    pairs_g = per_group // 2
    tpd = fin.shape[0]
    td = dfin.shape[0]
    zs = [lax.rem(z + s, groups) for s in range(1, groups)]
    zr = [lax.rem(z + groups - s, groups) for s in range(1, groups)]
    qs = [lax.rem(q + s, point_devs) for s in range(1, point_devs)]
    qr = [lax.rem(q + point_devs - s, point_devs) for s in range(1, point_devs)]

    barrier = pltpu.get_barrier_semaphore()
    for j in zs:
        pl.semaphore_signal(barrier, inc=1, device_id={"freq": j}, device_id_type=MESH)
    for j in qs:
        pl.semaphore_signal(barrier, inc=1, device_id={"pts": j}, device_id_type=MESH)
    pl.semaphore_wait(barrier, groups - 1 + point_devs - 1)

    def piece(owner, c):
        start = pl.multiple_of(owner * width + c * cw, 128)
        return spec_ref.at[:, :, :, pl.ds(start, cw)]

    def remote(src, dst, send, recv, axis, j):
        return pltpu.make_async_remote_copy(
            src_ref=src,
            dst_ref=dst,
            send_sem=send,
            recv_sem=recv,
            device_id={axis: j},
            device_id_type=MESH,
        )

    sends = []
    main = [[None] * (groups - 1) for _ in range(chunks)]
    for c in range(chunks):
        for s in range(groups - 1):
            copy = remote(
                piece(zs[s], c),
                bufs[c].at[pl.ds(z * f_dev, f_dev)],
                main_send.at[c, s],
                main_recv.at[c, s],
                "freq",
                zs[s],
            )
            copy.start()
            main[c][s] = copy
    own_copy = pltpu.make_async_copy(spec_ref, own, own_sem)
    own_copy.start()
    local_copies = []
    for c in range(chunks):
        copy = pltpu.make_async_copy(
            piece(z, c), bufs[c].at[pl.ds(z * f_dev, f_dev)], loc_sem.at[c]
        )
        copy.start()
        local_copies.append(copy)
    own_copy.wait()

    weights_row = w_ref[...]

    def density_body(i, carry):
        halves = []
        for h in range(2):
            rows = own[2 * i + h]
            real, imag = rows[0], rows[1]
            wr = (real.astype(f32) * weights_row).astype(bf16)
            wi = (imag.astype(f32) * weights_row).astype(bf16)
            halves.append(gram_pair(wr, wi, real, imag))
        out = jnp.concatenate(halves, axis=1) * (1.0 / (points * point_devs))
        dacc[pl.ds(i * 4, 4)] = out.reshape(4, 8, 128)
        return carry

    lax.fori_loop(0, f_dev // 2, density_body, 0)

    copies = []
    for s in range(point_devs - 1):
        copy = remote(
            dacc.at[pl.ds(qs[s] * td, td)], rd.at[s], d1_send.at[s], d1_recv.at[s], "pts", qs[s]
        )
        copy.start()
        copies.append(copy)
    for copy in copies:
        copy.wait()
    total = dacc[pl.ds(q * td, td)]
    for s in range(point_devs - 1):
        total = total + rd[s]
    dfin[...] = total
    dfull[pl.ds(q * td, td)] = total
    dens_gather = []
    for s in range(point_devs - 1):
        copy = remote(
            dfin, dfull.at[pl.ds(q * td, td)], d2_send.at[s], d2_recv.at[s], "pts", qs[s]
        )
        copy.start()
        dens_gather.append(copy)

    bis_scale = 1.0 / math.sqrt(blocks * points * point_devs)

    for c in range(chunks):
        local_copies[c].wait()
        for s in range(groups - 1):
            pltpu.make_async_copy(
                bufs[c].at[pl.ds(zr[s] * f_dev, f_dev)],
                bufs[c].at[pl.ds(zr[s] * f_dev, f_dev)],
                main_recv.at[c, s],
            ).wait()
        w_piece = w_ref[:, pl.ds(pl.multiple_of(z * width + c * cw, 128), cw)]
        buf = bufs[c]

        def triad_body(i, carry):
            halves = []
            for h in range(2):
                t = 2 * i + h
                k = tri_ref[t, 0]
                l = tri_ref[t, 1]
                m = jnp.where(k + l >= f_total, k + l - f_total, k + l)
                first = buf[k].astype(f32)
                second = buf[l].astype(f32)
                third = buf[m]
                pr = first[0] * second[0] - first[1] * second[1]
                pi = first[0] * second[1] + first[1] * second[0]
                pr = (pr * w_piece).astype(bf16)
                pi = (pi * w_piece).astype(bf16)
                halves.append(gram_pair(pr, pi, third[0], third[1]))
            out = jnp.concatenate(halves, axis=1).reshape(4, 8, 128)
            g = i // pairs_g
            at = (i - g * pairs_g) * 4
            if c == 0:
                acc[g, pl.ds(at, 4)] = out
            else:
                acc[g, pl.ds(at, 4)] += out
            return carry

        lax.fori_loop(0, triads // 2, triad_body, 0)

    copies = []
    for s in range(point_devs - 1):
        copy = remote(
            acc.at[:, pl.ds(qs[s] * tpd, tpd)], r1.at[s], r1_send.at[s], r1_recv.at[s], "pts", qs[s]
        )
        copy.start()
        copies.append(copy)
    for copy in dens_gather:
        copy.wait()
    dens_out[...] = dfull[...]
    for copy in copies:
        copy.wait()
    total = acc[:, pl.ds(q * tpd, tpd)]
    for s in range(point_devs - 1):
        total = total + r1[s]
    s1[...] = total
    copies = []
    for s in range(groups - 1):
        copy = remote(s1.at[zs[s]], r2.at[s], r2_send.at[s], r2_recv.at[s], "freq", zs[s])
        copy.start()
        copies.append(copy)
    for copy in copies:
        copy.wait()
    total = s1[z]
    for s in range(groups - 1):
        total = total + r2[s]
    total = total * bis_scale
    fin[...] = total
    full[pl.ds(q * tpd, tpd)] = total
    copies = []
    for s in range(point_devs - 1):
        copy = remote(
            fin, full.at[pl.ds(q * tpd, tpd)], r3_send.at[s], r3_recv.at[s], "pts", qs[s]
        )
        copy.start()
        copies.append(copy)
    for copy in copies:
        copy.wait()
    bis_out[...] = full[...]
    mat = full[...].reshape(pairs_g, 32, 128)

    lane_m = lane_in((pairs_g, 32, 128))
    low_m = lane_m < 64
    lane_v = lane_in((pairs_g, 1, 128))
    low_v = lane_v < 64
    real_v = lax.rem(lane_v, 64) < 32

    def apply(vec):
        va = jnp.where(real_v, vec, -vec)
        vb = swap_parts(vec, real_v)
        re0, re1 = segment_sum(mat * va, low_m)
        im0, im1 = segment_sum(mat * vb, low_m)
        return jnp.where(low_m, re0, re1), jnp.where(low_m, im0, im1)

    vec = jnp.where(real_v, 1.0 / math.sqrt(blocks), 0.0)
    for _ in range(ITERS):
        ur, ui = apply(vec)
        x = jnp.sum(mat * ur, axis=1, keepdims=True)
        y = jnp.sum(mat * ui, axis=1, keepdims=True)
        ys = swap_parts(y, real_v)
        w = jnp.where(real_v, x + ys, ys - x)
        n0, n1 = segment_sum(w * w, low_v)
        vec = w * (1.0 / jnp.sqrt(jnp.where(low_v, n0, n1) + 1.0))
    ur, ui = apply(vec)
    top = jnp.sum(ur * ur + ui * ui, axis=1, keepdims=True)
    n0, n1 = segment_sum(vec * vec, low_v)
    energy_out[...] = top / (blocks * (jnp.where(low_v, n0, n1) + 1.0))
    vec_out[...] = vec

    va = jnp.where(real_v, vec, -vec)
    vb = swap_parts(vec, real_v)
    row = lax.broadcasted_iota(jnp.int32, (8, 256), 0)
    col = lax.broadcasted_iota(jnp.int32, (8, 256), 1)
    keep = (col // 64) == (row // 2)
    even = lax.rem(row, 2) == 0
    for j in range(per_group // 4):
        a = jnp.concatenate([va[2 * j], va[2 * j + 1]], axis=1)
        b = jnp.concatenate([vb[2 * j], vb[2 * j + 1]], axis=1)
        block = jnp.where(keep, jnp.where(even, a, b), 0.0)
        lhs_mine[j] = block
        lhs_all[z, j] = block
    copies = []
    for s in range(groups - 1):
        copy = remote(lhs_mine, lhs_all.at[z], l_send.at[s], l_recv.at[s], "freq", zs[s])
        copy.start()
        copies.append(copy)

    def mode_rows(g, j, c):
        parts = []
        for i in range(4):
            t = g * per_group + j * 4 + i
            k = tri_ref[t, 0]
            l = tri_ref[t, 1]
            m = jnp.where(k + l >= f_total, k + l - f_total, k + l)
            parts.append(bufs[c][m].reshape(2 * blocks, cw))
        right = jnp.concatenate(parts, axis=0)
        return jnp.dot(lhs_all[g, j].astype(bf16), right, preferred_element_type=f32)

    for copy in copies:
        copy.wait()
    copies = []
    for s in range(groups - 1):
        g = zs[s]

        def mode_body(j, carry, g=g):
            for c in range(chunks):
                modes[g, pl.ds(pl.multiple_of(j * 8, 8), 8), c * cw : (c + 1) * cw] = mode_rows(
                    g, j, c
                )
            return carry

        lax.fori_loop(0, per_group // 4, mode_body, 0)
        copy = remote(
            modes.at[g],
            mode_buf.at[:, pl.ds(pl.multiple_of(z * width, 128), width)],
            m_send.at[s],
            m_recv.at[s],
            "freq",
            g,
        )
        copy.start()
        copies.append(copy)

    def own_mode_body(j, carry):
        for c in range(chunks):
            mode_buf[
                pl.ds(pl.multiple_of(j * 8, 8), 8),
                pl.ds(pl.multiple_of(z * width + c * cw, 128), cw),
            ] = mode_rows(z, j, c)
        return carry

    lax.fori_loop(0, per_group // 4, own_mode_body, 0)
    for c in range(chunks):
        for s in range(groups - 1):
            main[c][s].wait_send()
    for copy in copies:
        copy.wait()
    mode_out[...] = mode_buf[...]


def local(spectra, weights, triads):
    groups = lax.axis_size("freq")
    point_devs = lax.axis_size("pts")
    f_dev, _, blocks, points = spectra.shape
    tri_count = triads.shape[0]
    per_group = tri_count // groups
    pairs_g = per_group // 2
    width = points // groups
    chunks = width // 128
    cw = width // chunks
    tpd = pairs_g * 4 // point_devs
    td = f_dev // 2 * 4 // point_devs
    vmem = pl.BlockSpec(memory_space=pltpu.VMEM)
    dma = pltpu.SemaphoreType.DMA
    z1, p1 = groups - 1, point_devs - 1
    outs = pl.pallas_call(
        functools.partial(kernel, groups, point_devs, chunks),
        out_shape=[
            jax.ShapeDtypeStruct((pairs_g * 4, 8, 128), f32),
            jax.ShapeDtypeStruct((f_dev * 2, 8, 128), f32),
            jax.ShapeDtypeStruct((pairs_g, 1, 128), f32),
            jax.ShapeDtypeStruct((pairs_g, 1, 128), f32),
            jax.ShapeDtypeStruct((2 * per_group, points), f32),
        ],
        in_specs=[
            pl.BlockSpec(memory_space=pltpu.SMEM),
            vmem,
            pl.BlockSpec(memory_space=pl.ANY),
        ],
        out_specs=[vmem] * 5,
        scratch_shapes=[
            pltpu.VMEM(spectra.shape, bf16),
            pltpu.VMEM((groups, pairs_g * 4, 8, 128), f32),
            pltpu.VMEM((p1, groups, tpd, 8, 128), f32),
            pltpu.VMEM((groups, tpd, 8, 128), f32),
            pltpu.VMEM((z1, tpd, 8, 128), f32),
            pltpu.VMEM((tpd, 8, 128), f32),
            pltpu.VMEM((pairs_g * 4, 8, 128), f32),
            pltpu.VMEM((f_dev * 2, 8, 128), f32),
            pltpu.VMEM((p1, td, 8, 128), f32),
            pltpu.VMEM((td, 8, 128), f32),
            pltpu.VMEM((f_dev * 2, 8, 128), f32),
            pltpu.VMEM((per_group // 4, 8, 256), f32),
            pltpu.VMEM((groups, per_group // 4, 8, 256), f32),
            pltpu.VMEM((groups, 2 * per_group, width), f32),
            pltpu.VMEM((2 * per_group, points), f32),
            dma,
            dma((chunks,)),
            dma((chunks, z1)),
            dma((chunks, z1)),
            dma((p1,)),
            dma((p1,)),
            dma((p1,)),
            dma((p1,)),
            dma((p1,)),
            dma((p1,)),
            dma((z1,)),
            dma((z1,)),
            dma((p1,)),
            dma((p1,)),
            dma((z1,)),
            dma((z1,)),
            dma((z1,)),
            dma((z1,)),
        ]
        + [pltpu.VMEM((f_dev * groups, 2, blocks, cw), bf16)] * chunks,
        compiler_params=pltpu.CompilerParams(
            collective_id=0, has_side_effects=True, vmem_limit_bytes=56 * 1024 * 1024
        ),
    )(triads, weights.reshape(1, points), spectra)
    bis, dens, vec, energy, mode = outs
    bis = bis.reshape(pairs_g, 32, 2, 2, 32).transpose(0, 2, 3, 1, 4)
    dens = dens.reshape(f_dev // 2, 32, 2, 2, 32).transpose(0, 2, 3, 1, 4)
    return (
        bis.reshape(per_group, 2, 32, 32),
        dens.reshape(f_dev, 2, 32, 32),
        vec.reshape(per_group, 2, 32),
        energy.reshape(pairs_g, 2, 64)[:, :, 0].reshape(per_group),
        mode.reshape(per_group, 2, points),
    )


def solution(mesh):
    in_specs = (P("freq", None, None, "pts"), P("pts"), P())
    out_specs = (
        P("freq", None, None, None),
        P("freq", None, None, None),
        P("freq", None, None),
        P("freq"),
        P("freq", None, "pts"),
    )
    return jax.shard_map(local, mesh=mesh, in_specs=in_specs, out_specs=out_specs, check_vma=False)
```

```python
import functools
import math

import jax
import jax.numpy as jnp
from jax import lax
from jax.experimental import pallas as pl
from jax.experimental.pallas import tpu as pltpu
from jax.sharding import PartitionSpec as P

ITERS = 3
MESH = pl.DeviceIdType.MESH
f32 = jnp.float32
bf16 = jnp.bfloat16


def gram_pair(left_real, left_imag, right_real, right_imag):
    left = jnp.concatenate([left_real, left_imag], axis=1)
    right = jnp.concatenate(
        [
            jnp.concatenate([right_real, right_imag], axis=1),
            jnp.concatenate([right_imag, -right_real], axis=1),
        ],
        axis=0,
    )
    return lax.dot_general(left, right, (((1,), (1,)), ((), ())), preferred_element_type=f32)


def lane_in(shape):
    return lax.broadcasted_iota(jnp.int32, shape, len(shape) - 1)


def segment_sum(values, low):
    first = jnp.sum(jnp.where(low, values, 0.0), axis=-1, keepdims=True)
    second = jnp.sum(jnp.where(low, 0.0, values), axis=-1, keepdims=True)
    return first, second


def swap_parts(values, is_real):
    axis = values.ndim - 1
    up = pltpu.roll(values, 96, axis)
    down = pltpu.roll(values, 32, axis)
    return jnp.where(is_real, up, down)


def nearest_first(z, groups):
    table = []
    for me in range(groups):
        others = [j for j in range(groups) if j != me]
        inner = 1 if me < groups // 2 else -1
        table.append(sorted(others, key=lambda j: (abs(j - me), -(j - me) * inner)))
    peers = []
    for s in range(groups - 1):
        peer = table[0][s] + 0 * z
        for me in range(1, groups):
            peer = jnp.where(z == me, table[me][s], peer)
        peers.append(peer)
    return peers


def plan_kernel(groups, sizes, me_ref, tri_ref, slot_out, order_out, pick_out, need, rank):
    f_total = need.shape[0]
    f_dev = f_total // groups
    triads = tri_ref.shape[0]
    me = me_ref[0]

    def clear(f, carry):
        need[f] = 0
        return carry

    lax.fori_loop(0, f_total, clear, 0, unroll=8)

    def third_of(k, l):
        return jnp.where(k + l >= f_total, k + l - f_total, k + l)

    def mark(t, carry):
        k = tri_ref[t, 0]
        l = tri_ref[t, 1]
        need[k] = 1
        need[l] = 1
        need[third_of(k, l)] = 1
        return carry

    lax.fori_loop(0, triads, mark, 0, unroll=4)

    def fill(i, carry):
        order_out[i] = 0
        return carry

    lax.fori_loop(0, f_dev, fill, 0, unroll=8)

    def own_order(i, count):
        wanted = need[me * f_dev + i]

        @pl.when(wanted == 1)
        def _():
            order_out[count] = i

        return count + wanted

    lax.fori_loop(0, f_dev, own_order, 0, unroll=4)

    most = 0
    for g in range(groups):

        def count_body(i, count, g=g):
            rank[g * f_dev + i] = count
            return count + need[g * f_dev + i]

        most = jnp.maximum(most, lax.fori_loop(0, f_dev, count_body, 0, unroll=8))
    pick = 0
    stride = sizes[0]
    for i in range(len(sizes) - 1):
        over = most > sizes[i]
        pick = jnp.where(over, i + 1, pick)
        stride = jnp.where(over, sizes[i + 1], stride)
    pick_out[0] = pick

    def slots(t, carry):
        k = tri_ref[t, 0]
        l = tri_ref[t, 1]
        for i, f in enumerate((k, l, third_of(k, l))):
            slot_out[t, i] = (f // f_dev) * stride + rank[f]
        return carry

    lax.fori_loop(0, triads, slots, 0, unroll=4)


def kernel(
    groups,
    point_devs,
    chunks,
    tri_ref,
    order_ref,
    w_ref,
    spec_ref,
    bis_out,
    dens_out,
    vec_out,
    energy_out,
    mode_out,
    own,
    stage,
    acc,
    r1,
    s1,
    r2,
    fin,
    full,
    dacc,
    rd,
    dfin,
    dfull,
    lhs_mine,
    lhs_all,
    modes,
    mode_buf,
    own_sem,
    loc_sem,
    main_send,
    main_recv,
    d1_send,
    d1_recv,
    d2_send,
    d2_recv,
    r1_send,
    r1_recv,
    r2_send,
    r2_recv,
    r3_send,
    r3_recv,
    l_send,
    l_recv,
    m_send,
    m_recv,
    *bufs,
):
    z = lax.axis_index("freq")
    q = lax.axis_index("pts")
    f_dev, _, blocks, points = spec_ref.shape
    rows = stage.shape[0]
    width = points // groups
    cw = width // chunks
    triads = tri_ref.shape[0]
    per_group = triads // groups
    pairs_g = per_group // 2
    tpd = fin.shape[0]
    td = dfin.shape[0]
    zs = [lax.rem(z + s, groups) for s in range(1, groups)]
    near = nearest_first(z, groups)
    qs = [lax.rem(q + s, point_devs) for s in range(1, point_devs)]

    own_copy = pltpu.make_async_copy(spec_ref, own, own_sem)
    own_copy.start()
    barrier = pltpu.get_barrier_semaphore()
    for j in zs:
        pl.semaphore_signal(barrier, inc=1, device_id={"freq": j}, device_id_type=MESH)
    for j in qs:
        pl.semaphore_signal(barrier, inc=1, device_id={"pts": j}, device_id_type=MESH)
    pl.semaphore_wait(barrier, groups - 1 + point_devs - 1)

    def piece(owner, c):
        start = pl.multiple_of(owner * width + c * cw, 128)
        return stage.at[:, :, :, pl.ds(start, cw)]

    def remote(src, dst, send, recv, axis, j):
        return pltpu.make_async_remote_copy(
            src_ref=src,
            dst_ref=dst,
            send_sem=send,
            recv_sem=recv,
            device_id={axis: j},
            device_id_type=MESH,
        )

    own_copy.wait()

    def stage_body(i, carry):
        stage[i] = own[order_ref[i]]
        return carry

    lax.fori_loop(0, rows, stage_body, 0)

    main = []
    for s in range(groups - 1):
        for c in range(chunks):
            copy = remote(
                piece(near[s], c),
                bufs[c].at[pl.ds(z * rows, rows)],
                main_send.at[c, s],
                main_recv.at[c, z],
                "freq",
                near[s],
            )
            copy.start()
            main.append(copy)
    local_copies = []
    for c in range(chunks):
        copy = pltpu.make_async_copy(
            piece(z, c), bufs[c].at[pl.ds(z * rows, rows)], loc_sem.at[c]
        )
        copy.start()
        local_copies.append(copy)

    weights_row = w_ref[...]

    def density_body(i, carry):
        halves = []
        for h in range(2):
            rows = own[2 * i + h]
            real, imag = rows[0], rows[1]
            wr = (real.astype(f32) * weights_row).astype(bf16)
            wi = (imag.astype(f32) * weights_row).astype(bf16)
            halves.append(gram_pair(wr, wi, real, imag))
        out = jnp.concatenate(halves, axis=1) * (1.0 / (points * point_devs))
        dacc[pl.ds(i * 4, 4)] = out.reshape(4, 8, 128)
        return carry

    lax.fori_loop(0, f_dev // 2, density_body, 0)

    copies = []
    for s in range(point_devs - 1):
        copy = remote(
            dacc.at[pl.ds(qs[s] * td, td)], rd.at[s], d1_send.at[s], d1_recv.at[s], "pts", qs[s]
        )
        copy.start()
        copies.append(copy)
    for copy in copies:
        copy.wait()
    total = dacc[pl.ds(q * td, td)]
    for s in range(point_devs - 1):
        total = total + rd[s]
    dfin[...] = total
    dfull[pl.ds(q * td, td)] = total
    dens_gather = []
    for s in range(point_devs - 1):
        copy = remote(
            dfin, dfull.at[pl.ds(q * td, td)], d2_send.at[s], d2_recv.at[s], "pts", qs[s]
        )
        copy.start()
        dens_gather.append(copy)

    bis_scale = 1.0 / math.sqrt(blocks * points * point_devs)

    for c in range(chunks):
        local_copies[c].wait()
        for s in range(groups - 1):
            pltpu.make_async_copy(
                bufs[c].at[pl.ds(zs[s] * rows, rows)],
                bufs[c].at[pl.ds(zs[s] * rows, rows)],
                main_recv.at[c, zs[s]],
            ).wait()
        w_piece = w_ref[:, pl.ds(pl.multiple_of(z * width + c * cw, 128), cw)]
        buf = bufs[c]

        def triad_body(i, carry):
            halves = []
            for h in range(2):
                t = 2 * i + h
                first = buf[tri_ref[t, 0]].astype(f32)
                second = buf[tri_ref[t, 1]].astype(f32)
                third = buf[tri_ref[t, 2]]
                pr = first[0] * second[0] - first[1] * second[1]
                pi = first[0] * second[1] + first[1] * second[0]
                pr = (pr * w_piece).astype(bf16)
                pi = (pi * w_piece).astype(bf16)
                halves.append(gram_pair(pr, pi, third[0], third[1]))
            out = jnp.concatenate(halves, axis=1).reshape(4, 8, 128)
            g = i // pairs_g
            at = (i - g * pairs_g) * 4
            if c == 0:
                acc[g, pl.ds(at, 4)] = out
            else:
                acc[g, pl.ds(at, 4)] += out
            return carry

        if c < chunks - 1:
            lax.fori_loop(0, triads // 2, triad_body, 0)

    copies = []
    for g in range(groups):
        lax.fori_loop(g * pairs_g, (g + 1) * pairs_g, triad_body, 0)
        for s in range(point_devs - 1):
            copy = remote(
                acc.at[g, pl.ds(qs[s] * tpd, tpd)],
                r1.at[s, g],
                r1_send.at[s, g],
                r1_recv.at[s, g],
                "pts",
                qs[s],
            )
            copy.start()
            copies.append(copy)
    for copy in dens_gather:
        copy.wait()
    dens_out[...] = dfull[...]
    for copy in copies:
        copy.wait()
    total = acc[:, pl.ds(q * tpd, tpd)]
    for s in range(point_devs - 1):
        total = total + r1[s]
    s1[...] = total
    copies = []
    for s in range(groups - 1):
        copy = remote(s1.at[zs[s]], r2.at[s], r2_send.at[s], r2_recv.at[s], "freq", zs[s])
        copy.start()
        copies.append(copy)
    for copy in copies:
        copy.wait()
    total = s1[z]
    for s in range(groups - 1):
        total = total + r2[s]
    total = total * bis_scale
    fin[...] = total
    full[pl.ds(q * tpd, tpd)] = total
    copies = []
    for s in range(point_devs - 1):
        copy = remote(
            fin, full.at[pl.ds(q * tpd, tpd)], r3_send.at[s], r3_recv.at[s], "pts", qs[s]
        )
        copy.start()
        copies.append(copy)
    for copy in copies:
        copy.wait()
    bis_out[...] = full[...]
    mat = full[...].reshape(pairs_g, 32, 128)

    lane_m = lane_in((pairs_g, 32, 128))
    low_m = lane_m < 64
    lane_v = lane_in((pairs_g, 1, 128))
    low_v = lane_v < 64
    real_v = lax.rem(lane_v, 64) < 32

    def apply(vec):
        va = jnp.where(real_v, vec, -vec)
        vb = swap_parts(vec, real_v)
        re0, re1 = segment_sum(mat * va, low_m)
        im0, im1 = segment_sum(mat * vb, low_m)
        return jnp.where(low_m, re0, re1), jnp.where(low_m, im0, im1)

    vec = jnp.where(real_v, 1.0 / math.sqrt(blocks), 0.0)
    for _ in range(ITERS):
        ur, ui = apply(vec)
        x = jnp.sum(mat * ur, axis=1, keepdims=True)
        y = jnp.sum(mat * ui, axis=1, keepdims=True)
        ys = swap_parts(y, real_v)
        w = jnp.where(real_v, x + ys, ys - x)
        n0, n1 = segment_sum(w * w, low_v)
        vec = w * (1.0 / jnp.sqrt(jnp.where(low_v, n0, n1) + 1.0))
    ur, ui = apply(vec)
    top = jnp.sum(ur * ur + ui * ui, axis=1, keepdims=True)
    n0, n1 = segment_sum(vec * vec, low_v)
    energy_out[...] = top / (blocks * (jnp.where(low_v, n0, n1) + 1.0))
    vec_out[...] = vec

    va = jnp.where(real_v, vec, -vec)
    vb = swap_parts(vec, real_v)
    row = lax.broadcasted_iota(jnp.int32, (8, 256), 0)
    col = lax.broadcasted_iota(jnp.int32, (8, 256), 1)
    keep = (col // 64) == (row // 2)
    even = lax.rem(row, 2) == 0
    for j in range(per_group // 4):
        a = jnp.concatenate([va[2 * j], va[2 * j + 1]], axis=1)
        b = jnp.concatenate([vb[2 * j], vb[2 * j + 1]], axis=1)
        block = jnp.where(keep, jnp.where(even, a, b), 0.0)
        lhs_mine[j] = block
        lhs_all[z, j] = block
    copies = []
    for s in range(groups - 1):
        copy = remote(lhs_mine, lhs_all.at[z], l_send.at[s], l_recv.at[s], "freq", zs[s])
        copy.start()
        copies.append(copy)

    def mode_rows(g, j, c):
        parts = []
        for i in range(4):
            t = g * per_group + j * 4 + i
            parts.append(bufs[c][tri_ref[t, 2]].reshape(2 * blocks, cw))
        right = jnp.concatenate(parts, axis=0)
        return jnp.dot(lhs_all[g, j].astype(bf16), right, preferred_element_type=f32)

    for copy in copies:
        copy.wait()
    copies = []
    for s in range(groups - 1):
        g = zs[s]

        def mode_body(j, carry, g=g):
            for c in range(chunks):
                modes[g, pl.ds(pl.multiple_of(j * 8, 8), 8), c * cw : (c + 1) * cw] = mode_rows(
                    g, j, c
                )
            return carry

        lax.fori_loop(0, per_group // 4, mode_body, 0)
        copy = remote(
            modes.at[g],
            mode_buf.at[:, pl.ds(pl.multiple_of(z * width, 128), width)],
            m_send.at[s],
            m_recv.at[s],
            "freq",
            g,
        )
        copy.start()
        copies.append(copy)

    def own_mode_body(j, carry):
        for c in range(chunks):
            mode_buf[
                pl.ds(pl.multiple_of(j * 8, 8), 8),
                pl.ds(pl.multiple_of(z * width + c * cw, 128), cw),
            ] = mode_rows(z, j, c)
        return carry

    lax.fori_loop(0, per_group // 4, own_mode_body, 0)
    for copy in main:
        copy.wait_send()
    for copy in copies:
        copy.wait()
    mode_out[...] = mode_buf[...]


def local(spectra, weights, triads):
    groups = lax.axis_size("freq")
    point_devs = lax.axis_size("pts")
    f_dev, _, blocks, points = spectra.shape
    tri_count = triads.shape[0]
    per_group = tri_count // groups
    pairs_g = per_group // 2
    width = points // groups
    chunks = width // 128
    cw = width // chunks
    tpd = pairs_g * 4 // point_devs
    td = f_dev // 2 * 4 // point_devs
    vmem = pl.BlockSpec(memory_space=pltpu.VMEM)
    dma = pltpu.SemaphoreType.DMA
    z1, p1 = groups - 1, point_devs - 1
    sizes = sorted({-(-f_dev * n // 32) for n in (25, 26, 27, 28, 29, 32)})
    smem = pl.BlockSpec(memory_space=pltpu.SMEM)
    group_index = lax.axis_index("freq").astype(jnp.int32).reshape(1)
    slots, order, pick = pl.pallas_call(
        functools.partial(plan_kernel, groups, sizes),
        out_shape=[
            jax.ShapeDtypeStruct((tri_count, 3), jnp.int32),
            jax.ShapeDtypeStruct((f_dev,), jnp.int32),
            jax.ShapeDtypeStruct((1,), jnp.int32),
        ],
        in_specs=[smem, smem],
        out_specs=[smem] * 3,
        scratch_shapes=[
            pltpu.SMEM((f_dev * groups,), jnp.int32),
            pltpu.SMEM((f_dev * groups,), jnp.int32),
        ],
    )(group_index, triads)

    def run(branch, rows, slots, order, weights_row, spectra):
        return pl.pallas_call(
            functools.partial(kernel, groups, point_devs, chunks),
            out_shape=[
                jax.ShapeDtypeStruct((pairs_g * 4, 8, 128), f32),
                jax.ShapeDtypeStruct((f_dev * 2, 8, 128), f32),
                jax.ShapeDtypeStruct((pairs_g, 1, 128), f32),
                jax.ShapeDtypeStruct((pairs_g, 1, 128), f32),
                jax.ShapeDtypeStruct((2 * per_group, points), f32),
            ],
            in_specs=[
                pl.BlockSpec(memory_space=pltpu.SMEM),
                pl.BlockSpec(memory_space=pltpu.SMEM),
                vmem,
                pl.BlockSpec(memory_space=pl.ANY),
            ],
            out_specs=[vmem] * 5,
            scratch_shapes=[
                pltpu.VMEM(spectra.shape, bf16),
                pltpu.VMEM((rows,) + spectra.shape[1:], bf16),
                pltpu.VMEM((groups, pairs_g * 4, 8, 128), f32),
                pltpu.VMEM((p1, groups, tpd, 8, 128), f32),
                pltpu.VMEM((groups, tpd, 8, 128), f32),
                pltpu.VMEM((z1, tpd, 8, 128), f32),
                pltpu.VMEM((tpd, 8, 128), f32),
                pltpu.VMEM((pairs_g * 4, 8, 128), f32),
                pltpu.VMEM((f_dev * 2, 8, 128), f32),
                pltpu.VMEM((p1, td, 8, 128), f32),
                pltpu.VMEM((td, 8, 128), f32),
                pltpu.VMEM((f_dev * 2, 8, 128), f32),
                pltpu.VMEM((per_group // 4, 8, 256), f32),
                pltpu.VMEM((groups, per_group // 4, 8, 256), f32),
                pltpu.VMEM((groups, 2 * per_group, width), f32),
                pltpu.VMEM((2 * per_group, points), f32),
                dma,
                dma((chunks,)),
                dma((chunks, z1)),
                dma((chunks, groups)),
                dma((p1,)),
                dma((p1,)),
                dma((p1,)),
                dma((p1,)),
                dma((p1, groups)),
                dma((p1, groups)),
                dma((z1,)),
                dma((z1,)),
                dma((p1,)),
                dma((p1,)),
                dma((z1,)),
                dma((z1,)),
                dma((z1,)),
                dma((z1,)),
            ]
            + [pltpu.VMEM((rows * groups, 2, blocks, cw), bf16)] * chunks,
            compiler_params=pltpu.CompilerParams(
                collective_id=branch, has_side_effects=True, vmem_limit_bytes=56 * 1024 * 1024
            ),
        )(slots, order, weights_row, spectra)

    outs = lax.switch(
        pick[0],
        [functools.partial(run, i, n) for i, n in enumerate(sizes)],
        slots,
        order,
        weights.reshape(1, points),
        spectra,
    )
    bis, dens, vec, energy, mode = outs
    bis = bis.reshape(pairs_g, 32, 2, 2, 32).transpose(0, 2, 3, 1, 4)
    dens = dens.reshape(f_dev // 2, 32, 2, 2, 32).transpose(0, 2, 3, 1, 4)
    return (
        bis.reshape(per_group, 2, 32, 32),
        dens.reshape(f_dev, 2, 32, 32),
        vec.reshape(per_group, 2, 32),
        energy.reshape(pairs_g, 2, 64)[:, :, 0].reshape(per_group),
        mode.reshape(per_group, 2, points),
    )


def solution(mesh):
    in_specs = (P("freq", None, None, "pts"), P("pts"), P())
    out_specs = (
        P("freq", None, None, None),
        P("freq", None, None, None),
        P("freq", None, None),
        P("freq"),
        P("freq", None, "pts"),
    )
    return jax.shard_map(local, mesh=mesh, in_specs=in_specs, out_specs=out_specs, check_vma=False)
```

```python
import functools
import math

import jax
import jax.numpy as jnp
from jax import lax
from jax.experimental import pallas as pl
from jax.experimental.pallas import tpu as pltpu
from jax.sharding import PartitionSpec as P

ITERS = 3
MESH = pl.DeviceIdType.MESH
f32 = jnp.float32
bf16 = jnp.bfloat16


def gram_pair(left_real, left_imag, right_real, right_imag):
    left = jnp.concatenate([left_real, left_imag], axis=1)
    right = jnp.concatenate(
        [
            jnp.concatenate([right_real, right_imag], axis=1),
            jnp.concatenate([right_imag, -right_real], axis=1),
        ],
        axis=0,
    )
    return lax.dot_general(left, right, (((1,), (1,)), ((), ())), preferred_element_type=f32)


def lane_in(shape):
    return lax.broadcasted_iota(jnp.int32, shape, len(shape) - 1)


def segment_sum(values, low):
    first = jnp.sum(jnp.where(low, values, 0.0), axis=-1, keepdims=True)
    second = jnp.sum(jnp.where(low, 0.0, values), axis=-1, keepdims=True)
    return first, second


def swap_parts(values, is_real):
    axis = values.ndim - 1
    up = pltpu.roll(values, 96, axis)
    down = pltpu.roll(values, 32, axis)
    return jnp.where(is_real, up, down)


def nearest_first(z, groups):
    table = []
    for me in range(groups):
        others = [j for j in range(groups) if j != me]
        inner = 1 if me < groups // 2 else -1
        table.append(sorted(others, key=lambda j: (abs(j - me), -(j - me) * inner)))
    peers = []
    for s in range(groups - 1):
        peer = table[0][s] + 0 * z
        for me in range(1, groups):
            peer = jnp.where(z == me, table[me][s], peer)
        peers.append(peer)
    return peers


def plan_kernel(groups, sizes, me_ref, tri_ref, slot_out, order_out, pick_out, need, rank):
    f_total = need.shape[0]
    f_dev = f_total // groups
    triads = tri_ref.shape[0]
    me = me_ref[0]

    def clear(f, carry):
        need[f] = 0
        return carry

    lax.fori_loop(0, f_total, clear, 0, unroll=8)

    def third_of(k, l):
        return jnp.where(k + l >= f_total, k + l - f_total, k + l)

    def mark(t, carry):
        k = tri_ref[t, 0]
        l = tri_ref[t, 1]
        need[k] = 1
        need[l] = 1
        need[third_of(k, l)] = 1
        return carry

    lax.fori_loop(0, triads, mark, 0, unroll=4)

    def fill(i, carry):
        order_out[i] = 0
        return carry

    lax.fori_loop(0, f_dev, fill, 0, unroll=8)

    def own_order(i, count):
        wanted = need[me * f_dev + i]

        @pl.when(wanted == 1)
        def _():
            order_out[count] = i

        return count + wanted

    lax.fori_loop(0, f_dev, own_order, 0, unroll=4)

    most = 0
    for g in range(groups):

        def count_body(i, count, g=g):
            rank[g * f_dev + i] = count
            return count + need[g * f_dev + i]

        most = jnp.maximum(most, lax.fori_loop(0, f_dev, count_body, 0, unroll=8))
    pick = 0
    stride = sizes[0]
    for i in range(len(sizes) - 1):
        over = most > sizes[i]
        pick = jnp.where(over, i + 1, pick)
        stride = jnp.where(over, sizes[i + 1], stride)
    pick_out[0] = pick

    def slots(t, carry):
        k = tri_ref[t, 0]
        l = tri_ref[t, 1]
        for i, f in enumerate((k, l, third_of(k, l))):
            slot_out[t, i] = (f // f_dev) * stride + rank[f]
        return carry

    lax.fori_loop(0, triads, slots, 0, unroll=4)


def kernel(
    groups,
    point_devs,
    chunks,
    tri_ref,
    order_ref,
    w_ref,
    spec_ref,
    bis_out,
    dens_out,
    vec_out,
    energy_out,
    mode_out,
    own,
    stage,
    acc,
    r1,
    s1,
    r2,
    fin,
    full,
    dacc,
    rd,
    dfin,
    dfull,
    lhs_mine,
    lhs_all,
    modes,
    mode_buf,
    own_sem,
    loc_sem,
    main_send,
    main_recv,
    d1_send,
    d1_recv,
    d2_send,
    d2_recv,
    r1_send,
    r1_recv,
    r2_send,
    r2_recv,
    r3_send,
    r3_recv,
    l_send,
    l_recv,
    m_send,
    m_recv,
    *bufs,
):
    z = lax.axis_index("freq")
    q = lax.axis_index("pts")
    f_dev, _, blocks, points = spec_ref.shape
    rows = stage.shape[0]
    width = points // groups
    cw = width // chunks
    triads = tri_ref.shape[0]
    per_group = triads // groups
    pairs_g = per_group // 2
    tpd = fin.shape[0]
    td = dfin.shape[0]
    zs = [lax.rem(z + s, groups) for s in range(1, groups)]
    near = nearest_first(z, groups)
    qs = [lax.rem(q + s, point_devs) for s in range(1, point_devs)]

    own_copy = pltpu.make_async_copy(spec_ref, own, own_sem)
    own_copy.start()
    barrier = pltpu.get_barrier_semaphore()
    for j in zs:
        pl.semaphore_signal(barrier, inc=1, device_id={"freq": j}, device_id_type=MESH)
    for j in qs:
        pl.semaphore_signal(barrier, inc=1, device_id={"pts": j}, device_id_type=MESH)
    pl.semaphore_wait(barrier, groups - 1 + point_devs - 1)

    def piece(owner, c):
        start = pl.multiple_of(owner * width + c * cw, 128)
        return stage.at[:, :, :, pl.ds(start, cw)]

    def remote(src, dst, send, recv, axis, j):
        return pltpu.make_async_remote_copy(
            src_ref=src,
            dst_ref=dst,
            send_sem=send,
            recv_sem=recv,
            device_id={axis: j},
            device_id_type=MESH,
        )

    own_copy.wait()

    def stage_body(i, carry):
        stage[i] = own[order_ref[i]]
        return carry

    lax.fori_loop(0, rows, stage_body, 0)

    main = []
    for s in range(groups - 1):
        for c in range(chunks):
            copy = remote(
                piece(near[s], c),
                bufs[c].at[pl.ds(z * rows, rows)],
                main_send.at[c, s],
                main_recv.at[c, z],
                "freq",
                near[s],
            )
            copy.start()
            main.append(copy)
    local_copies = []
    for c in range(chunks):
        copy = pltpu.make_async_copy(
            piece(z, c), bufs[c].at[pl.ds(z * rows, rows)], loc_sem.at[c]
        )
        copy.start()
        local_copies.append(copy)

    weights_row = w_ref[...]

    def density_body(i, carry):
        halves = []
        for h in range(2):
            rows = own[2 * i + h]
            real, imag = rows[0], rows[1]
            wr = (real.astype(f32) * weights_row).astype(bf16)
            wi = (imag.astype(f32) * weights_row).astype(bf16)
            halves.append(gram_pair(wr, wi, real, imag))
        out = jnp.concatenate(halves, axis=1) * (1.0 / (points * point_devs))
        dacc[pl.ds(i * 4, 4)] = out.reshape(4, 8, 128)
        return carry

    lax.fori_loop(0, f_dev // 2, density_body, 0)

    copies = []
    for s in range(point_devs - 1):
        copy = remote(
            dacc.at[pl.ds(qs[s] * td, td)], rd.at[s], d1_send.at[s], d1_recv.at[s], "pts", qs[s]
        )
        copy.start()
        copies.append(copy)
    for copy in copies:
        copy.wait()
    total = dacc[pl.ds(q * td, td)]
    for s in range(point_devs - 1):
        total = total + rd[s]
    dfin[...] = total
    dfull[pl.ds(q * td, td)] = total
    dens_gather = []
    for s in range(point_devs - 1):
        copy = remote(
            dfin, dfull.at[pl.ds(q * td, td)], d2_send.at[s], d2_recv.at[s], "pts", qs[s]
        )
        copy.start()
        dens_gather.append(copy)

    bis_scale = 1.0 / math.sqrt(blocks * points * point_devs)

    for c in range(chunks):
        local_copies[c].wait()
        for s in range(groups - 1):
            pltpu.make_async_copy(
                bufs[c].at[pl.ds(zs[s] * rows, rows)],
                bufs[c].at[pl.ds(zs[s] * rows, rows)],
                main_recv.at[c, zs[s]],
            ).wait()
        w_piece = w_ref[:, pl.ds(pl.multiple_of(z * width + c * cw, 128), cw)]
        buf = bufs[c]

        def triad_body(i, carry):
            halves = []
            for h in range(2):
                t = 2 * i + h
                first = buf[tri_ref[t, 0]].astype(f32)
                second = buf[tri_ref[t, 1]].astype(f32)
                third = buf[tri_ref[t, 2]]
                pr = first[0] * second[0] - first[1] * second[1]
                pi = first[0] * second[1] + first[1] * second[0]
                pr = (pr * w_piece).astype(bf16)
                pi = (pi * w_piece).astype(bf16)
                halves.append(gram_pair(pr, pi, third[0], third[1]))
            out = jnp.concatenate(halves, axis=1).reshape(4, 8, 128)
            g = i // pairs_g
            at = (i - g * pairs_g) * 4
            if c == 0:
                acc[g, pl.ds(at, 4)] = out
            else:
                acc[g, pl.ds(at, 4)] += out
            return carry

        if c < chunks - 1:
            lax.fori_loop(0, triads // 2, triad_body, 0)

    copies = []
    for g in range(groups):
        lax.fori_loop(g * pairs_g, (g + 1) * pairs_g, triad_body, 0)
        for s in range(point_devs - 1):
            copy = remote(
                acc.at[g, pl.ds(qs[s] * tpd, tpd)],
                r1.at[s, g],
                r1_send.at[s, g],
                r1_recv.at[s, g],
                "pts",
                qs[s],
            )
            copy.start()
            copies.append(copy)
    for copy in dens_gather:
        copy.wait()
    dens_out[...] = dfull[...]
    for copy in copies:
        copy.wait()
    total = acc[:, pl.ds(q * tpd, tpd)]
    for s in range(point_devs - 1):
        total = total + r1[s]
    s1[...] = total
    copies = []
    for s in range(groups - 1):
        copy = remote(s1.at[zs[s]], r2.at[s], r2_send.at[s], r2_recv.at[s], "freq", zs[s])
        copy.start()
        copies.append(copy)
    for copy in copies:
        copy.wait()
    total = s1[z]
    for s in range(groups - 1):
        total = total + r2[s]
    total = total * bis_scale
    fin[...] = total
    full[pl.ds(q * tpd, tpd)] = total
    copies = []
    for s in range(point_devs - 1):
        copy = remote(
            fin, full.at[pl.ds(q * tpd, tpd)], r3_send.at[s], r3_recv.at[s], "pts", qs[s]
        )
        copy.start()
        copies.append(copy)
    for copy in copies:
        copy.wait()
    mat = full[...].reshape(pairs_g, 32, 128)

    lane_m = lane_in((pairs_g, 32, 128))
    low_m = lane_m < 64
    lane_v = lane_in((pairs_g, 1, 128))
    low_v = lane_v < 64
    real_v = lax.rem(lane_v, 64) < 32

    def apply(vec):
        va = jnp.where(real_v, vec, -vec)
        vb = swap_parts(vec, real_v)
        re0, re1 = segment_sum(mat * va, low_m)
        im0, im1 = segment_sum(mat * vb, low_m)
        return jnp.where(low_m, re0, re1), jnp.where(low_m, im0, im1)

    vec = jnp.where(real_v, 1.0 / math.sqrt(blocks), 0.0)
    for _ in range(ITERS):
        ur, ui = apply(vec)
        x = jnp.sum(mat * ur, axis=1, keepdims=True)
        y = jnp.sum(mat * ui, axis=1, keepdims=True)
        ys = swap_parts(y, real_v)
        w = jnp.where(real_v, x + ys, ys - x)
        n0, n1 = segment_sum(w * w, low_v)
        vec = w * (1.0 / jnp.sqrt(jnp.where(low_v, n0, n1) + 1.0))
    ur, ui = apply(vec)
    top = jnp.sum(ur * ur + ui * ui, axis=1, keepdims=True)
    n0, n1 = segment_sum(vec * vec, low_v)
    energy_out[...] = top / (blocks * (jnp.where(low_v, n0, n1) + 1.0))
    vec_out[...] = vec

    va = jnp.where(real_v, vec, -vec)
    vb = swap_parts(vec, real_v)
    row = lax.broadcasted_iota(jnp.int32, (8, 256), 0)
    col = lax.broadcasted_iota(jnp.int32, (8, 256), 1)
    keep = (col // 64) == (row // 2)
    even = lax.rem(row, 2) == 0
    for j in range(per_group // 4):
        a = jnp.concatenate([va[2 * j], va[2 * j + 1]], axis=1)
        b = jnp.concatenate([vb[2 * j], vb[2 * j + 1]], axis=1)
        block = jnp.where(keep, jnp.where(even, a, b), 0.0)
        lhs_mine[j] = block
        lhs_all[z, j] = block
    copies = []
    for s in range(groups - 1):
        copy = remote(lhs_mine, lhs_all.at[z], l_send.at[s], l_recv.at[s], "freq", zs[s])
        copy.start()
        copies.append(copy)

    def mode_rows(g, j, c):
        parts = []
        for i in range(4):
            t = g * per_group + j * 4 + i
            parts.append(bufs[c][tri_ref[t, 2]].reshape(2 * blocks, cw))
        right = jnp.concatenate(parts, axis=0)
        return jnp.dot(lhs_all[g, j].astype(bf16), right, preferred_element_type=f32)

    def two_blocks(g, j, c):
        pair = [mode_rows(g, 2 * j, c), mode_rows(g, 2 * j + 1, c)]
        return jnp.concatenate(pair, axis=0).astype(bf16)

    bis_out[...] = full[...]
    for copy in copies:
        copy.wait()
    copies = []
    for s in range(groups - 1):
        g = zs[s]

        def mode_body(j, carry, g=g):
            for c in range(chunks):
                modes[g, pl.ds(pl.multiple_of(j * 16, 16), 16), c * cw : (c + 1) * cw] = two_blocks(
                    g, j, c
                )
            return carry

        lax.fori_loop(0, per_group // 8, mode_body, 0)
        copy = remote(
            modes.at[g],
            mode_buf.at[:, pl.ds(pl.multiple_of(z * width, 128), width)],
            m_send.at[s],
            m_recv.at[s],
            "freq",
            g,
        )
        copy.start()
        copies.append(copy)

    def own_mode_body(j, carry):
        for c in range(chunks):
            mode_buf[
                pl.ds(pl.multiple_of(j * 16, 16), 16),
                pl.ds(pl.multiple_of(z * width + c * cw, 128), cw),
            ] = two_blocks(z, j, c)
        return carry

    lax.fori_loop(0, per_group // 8, own_mode_body, 0)
    for copy in main:
        copy.wait_send()
    for copy in copies:
        copy.wait()
    mode_out[...] = mode_buf[...].astype(f32)


def local(spectra, weights, triads):
    groups = lax.axis_size("freq")
    point_devs = lax.axis_size("pts")
    f_dev, _, blocks, points = spectra.shape
    tri_count = triads.shape[0]
    per_group = tri_count // groups
    pairs_g = per_group // 2
    width = points // groups
    chunks = width // 128
    cw = width // chunks
    tpd = pairs_g * 4 // point_devs
    td = f_dev // 2 * 4 // point_devs
    vmem = pl.BlockSpec(memory_space=pltpu.VMEM)
    dma = pltpu.SemaphoreType.DMA
    z1, p1 = groups - 1, point_devs - 1
    sizes = sorted({-(-f_dev * n // 32) for n in (25, 26, 27, 28, 29, 32)})
    smem = pl.BlockSpec(memory_space=pltpu.SMEM)
    group_index = lax.axis_index("freq").astype(jnp.int32).reshape(1)
    slots, order, pick = pl.pallas_call(
        functools.partial(plan_kernel, groups, sizes),
        out_shape=[
            jax.ShapeDtypeStruct((tri_count, 3), jnp.int32),
            jax.ShapeDtypeStruct((f_dev,), jnp.int32),
            jax.ShapeDtypeStruct((1,), jnp.int32),
        ],
        in_specs=[smem, smem],
        out_specs=[smem] * 3,
        scratch_shapes=[
            pltpu.SMEM((f_dev * groups,), jnp.int32),
            pltpu.SMEM((f_dev * groups,), jnp.int32),
        ],
    )(group_index, triads)

    def run(branch, rows, slots, order, weights_row, spectra):
        return pl.pallas_call(
            functools.partial(kernel, groups, point_devs, chunks),
            out_shape=[
                jax.ShapeDtypeStruct((pairs_g * 4, 8, 128), f32),
                jax.ShapeDtypeStruct((f_dev * 2, 8, 128), f32),
                jax.ShapeDtypeStruct((pairs_g, 1, 128), f32),
                jax.ShapeDtypeStruct((pairs_g, 1, 128), f32),
                jax.ShapeDtypeStruct((2 * per_group, points), f32),
            ],
            in_specs=[
                pl.BlockSpec(memory_space=pltpu.SMEM),
                pl.BlockSpec(memory_space=pltpu.SMEM),
                vmem,
                pl.BlockSpec(memory_space=pl.ANY),
            ],
            out_specs=[vmem] * 5,
            scratch_shapes=[
                pltpu.VMEM(spectra.shape, bf16),
                pltpu.VMEM((rows,) + spectra.shape[1:], bf16),
                pltpu.VMEM((groups, pairs_g * 4, 8, 128), f32),
                pltpu.VMEM((p1, groups, tpd, 8, 128), f32),
                pltpu.VMEM((groups, tpd, 8, 128), f32),
                pltpu.VMEM((z1, tpd, 8, 128), f32),
                pltpu.VMEM((tpd, 8, 128), f32),
                pltpu.VMEM((pairs_g * 4, 8, 128), f32),
                pltpu.VMEM((f_dev * 2, 8, 128), f32),
                pltpu.VMEM((p1, td, 8, 128), f32),
                pltpu.VMEM((td, 8, 128), f32),
                pltpu.VMEM((f_dev * 2, 8, 128), f32),
                pltpu.VMEM((per_group // 4, 8, 256), f32),
                pltpu.VMEM((groups, per_group // 4, 8, 256), f32),
                pltpu.VMEM((groups, 2 * per_group, width), bf16),
                pltpu.VMEM((2 * per_group, points), bf16),
                dma,
                dma((chunks,)),
                dma((chunks, z1)),
                dma((chunks, groups)),
                dma((p1,)),
                dma((p1,)),
                dma((p1,)),
                dma((p1,)),
                dma((p1, groups)),
                dma((p1, groups)),
                dma((z1,)),
                dma((z1,)),
                dma((p1,)),
                dma((p1,)),
                dma((z1,)),
                dma((z1,)),
                dma((z1,)),
                dma((z1,)),
            ]
            + [pltpu.VMEM((rows * groups, 2, blocks, cw), bf16)] * chunks,
            compiler_params=pltpu.CompilerParams(
                collective_id=branch, has_side_effects=True, vmem_limit_bytes=56 * 1024 * 1024
            ),
        )(slots, order, weights_row, spectra)

    outs = lax.switch(
        pick[0],
        [functools.partial(run, i, n) for i, n in enumerate(sizes)],
        slots,
        order,
        weights.reshape(1, points),
        spectra,
    )
    bis, dens, vec, energy, mode = outs
    bis = bis.reshape(pairs_g, 32, 2, 2, 32).transpose(0, 2, 3, 1, 4)
    dens = dens.reshape(f_dev // 2, 32, 2, 2, 32).transpose(0, 2, 3, 1, 4)
    return (
        bis.reshape(per_group, 2, 32, 32),
        dens.reshape(f_dev, 2, 32, 32),
        vec.reshape(per_group, 2, 32),
        energy.reshape(pairs_g, 2, 64)[:, :, 0].reshape(per_group),
        mode.reshape(per_group, 2, points),
    )


def solution(mesh):
    in_specs = (P("freq", None, None, "pts"), P("pts"), P())
    out_specs = (
        P("freq", None, None, None),
        P("freq", None, None, None),
        P("freq", None, None),
        P("freq"),
        P("freq", None, "pts"),
    )
    return jax.shard_map(local, mesh=mesh, in_specs=in_specs, out_specs=out_specs, check_vma=False)
```
